8 devices in a mesh: rep: 1 (over z), dp: 8 (over x, y, core).
Axes of the slice: x: 2, y: 2, z: 1, core: 2. Of those that a mesh axis runs over, the one named last changes fastest.
Arguments:
- x: bfloat16 [8, 2048, 1152], P(('rep', 'dp'))
- dy: bfloat16 [8, 2048, 1152], P(('rep', 'dp'))
- w_gate: bfloat16 [2, 1152, 4608], P(None, 'dp')
- w_up: bfloat16 [2, 1152, 4608], P(None, 'dp')
- w_down: bfloat16 [2, 4608, 1152], P(None, 'dp')
Outputs:
- output 1: bfloat16 [8, 2048, 1152], P(('rep', 'dp'))
- output 2: bfloat16 [2, 1152, 4608], P('rep', 'dp')
- output 3: bfloat16 [2, 1152, 4608], P('rep', 'dp')
- output 4: bfloat16 [2, 4608, 1152], P('rep', 'dp')
All inputs are finite; a program needn't handle non-finite values.
Results may differ from the reference program's by a relative error of at most 0.018.
Values are sent between devices in bfloat16 or wider.
A program may use at most 2 GiB of HBM per device.

```python
import jax
import jax.numpy as jnp
from jax import lax

SEQUENCES = 8
TOKENS = 2048
D = 1152
FF = 4608
LAYERS = 2
NAMES = ("w_gate", "w_up", "w_down")
SHAPES = {"w_gate": (LAYERS, D, FF), "w_up": (LAYERS, D, FF), "w_down": (LAYERS, FF, D)}


def bump(key, n, height):
    away = (jnp.arange(n, dtype=jnp.int32) - jax.random.randint(key, (), 0, n, jnp.int32)) % n
    return jnp.where(away < n // 8, height, 1.0)


def together(key, own, strength):
    shared = jax.random.normal(key, own.shape[1:], jnp.float32)
    return (own + strength * shared) * lax.rsqrt(1 + strength * strength)


def setup_inputs(seed: int = 0, part: int = 0) -> dict:
    kx, kdy, ka, kb, kz, kf, kh, kl, *kw = jax.random.split(jax.random.key(seed), 8 + len(NAMES))
    kx, kdy, ka, kb = (jax.random.fold_in(k, part) for k in (kx, kdy, ka, kb))
    shape = (SEQUENCES, TOKENS, D)
    much_x, much_dy = jax.random.uniform(kz, (2,), jnp.float32, 0.0, 1.0)
    layers = 2.0 ** jax.random.uniform(kl, (LAYERS, 1, 1), jnp.float32, -1.0, 1.0)
    x = together(ka, jax.random.normal(kx, shape, jnp.float32), much_x) * bump(kf, D, 4.0)
    dy = together(kb, jax.random.normal(kdy, shape, jnp.float32), much_dy)
    drawn = {"x": x.astype(jnp.bfloat16), "dy": (dy * (SEQUENCES * TOKENS) ** -0.5).astype(jnp.bfloat16)}
    for key, name in zip(kw, NAMES, strict=True):
        w = jax.random.normal(key, SHAPES[name], jnp.float32) * SHAPES[name][1] ** -0.5
        drawn[name] = (w * {"w_gate": 1.0, "w_up": bump(kh, FF, 4.0), "w_down": layers}[name]).astype(jnp.bfloat16)
    return drawn


def matmul(a, w):
    return jnp.dot(a, w, preferred_element_type=jnp.float32).astype(jnp.bfloat16)


def normed(h):
    wide = h.astype(jnp.float32)
    scale = lax.rsqrt(jnp.mean(wide**2, -1, keepdims=True) + 1e-6)
    return (wide * scale).astype(jnp.bfloat16)


def layer(h, w):
    a = normed(h)
    gate = jnp.dot(a, w["w_gate"], preferred_element_type=jnp.float32)
    up = jnp.dot(a, w["w_up"], preferred_element_type=jnp.float32)
    return h + matmul((jax.nn.silu(gate) * up).astype(jnp.bfloat16), w["w_down"])


def stack(weights, h):
    return lax.scan(lambda h, w: (layer(h, w), None), h, weights)[0]


def reference(x, dy, w_gate, w_up, w_down):
    weights = dict(zip(NAMES, (w_gate, w_up, w_down), strict=True))

    def take(so_far, sequence):
        h, by_y = sequence
        _, back = jax.vjp(stack, weights, h)
        by_weights, by_h = back(by_y)
        return jax.tree.map(lambda total, term: total + term.astype(jnp.float32), so_far, by_weights), by_h

    none_yet = {name: jnp.zeros(w.shape, jnp.float32) for name, w in weights.items()}
    by_weights, by_x = lax.scan(take, none_yet, (x, dy))
    return (by_x, *(by_weights[name].astype(jnp.bfloat16) for name in NAMES))
```

```python
import functools

import jax
import jax.numpy as jnp
from jax import lax
from jax.experimental import pallas as pl
from jax.experimental.pallas import tpu as pltpu
from jax.sharding import PartitionSpec as P


T, D, FF = 2048, 1152, 4608
HALF = FF // 2
RD = D // 8
RF = FF // 8
BF, F32 = jnp.bfloat16, jnp.float32
VMEM_LIMIT = 60 * 1024 * 1024
NT = (((1,), (1,)), ((), ()))
TN = (((0,), (0,)), ((), ()))
ANY = pl.BlockSpec(memory_space=pl.ANY)


def first(i):
    return i ^ (4 if i % 2 == 0 else 2)


def second(i):
    return i ^ (2 if i % 2 == 0 else 4)


def partner(i):
    return i ^ 1


def send(v, to):
    return lax.ppermute(v, "dp", [(i, to(i)) for i in range(8)])


def dot(a, b, dims=None):
    if dims is None:
        return jnp.dot(a, b, preferred_element_type=F32)
    return lax.dot_general(a, b, dims, preferred_element_type=F32)


def params(**kw):
    return pltpu.CompilerParams(vmem_limit_bytes=VMEM_LIMIT, **kw)


def cost(flops, nbytes):
    return pl.CostEstimate(flops=flops, bytes_accessed=nbytes, transcendentals=0)


def places():
    me = lax.axis_index("dp")
    core = me % 2
    one, two = 4 - 2 * core, 2 + 2 * core
    other = me ^ 1
    where = [me, me ^ one, me ^ two, me ^ 6, other, other ^ two, other ^ one, other ^ 6]
    slots = []
    for b in range(8):
        chips = (b ^ me) // 2
        ahead = 2 if b % 2 == 0 else 1
        slot = jnp.where(chips == 0, 0, jnp.where(chips == 3, 1, jnp.where(chips == ahead, 2, 3)))
        slots.append(slot + 4 * ((b ^ me) % 2))
    return jnp.stack([v.astype(jnp.int32) for v in (*where, *slots)])


GU_M, GU_N, GU_C = 512, 768, 128
GU_STEPS = HALF // GU_N


def gu_body(pos, a_ref, *refs):
    blocks, (act_ref, s_ref, t_ref, wg, wu, sem) = refs[:8], refs[8:]
    n, m = pl.program_id(0), pl.program_id(1)

    def copies(k):
        cols = pl.ds(k * GU_N, GU_N)
        out = []
        for j, block in enumerate(blocks):
            rows = pl.ds(pl.multiple_of(pos[j] * RD, 16), RD)
            out.append(pltpu.make_async_copy(block.at[pl.ds(0, RD), cols], wg.at[k, rows, :], sem.at[k, 2 * j]))
            out.append(pltpu.make_async_copy(block.at[pl.ds(RD, RD), cols], wu.at[k, rows, :], sem.at[k, 2 * j + 1]))
        return out

    @pl.when((n == 0) & (m == 0))
    def _():
        for k in range(GU_STEPS):
            for c in copies(k):
                c.start()

    for k in range(GU_STEPS):

        @pl.when((n == k) & (m == 0))
        def _():
            for c in copies(k):
                c.wait()

    for c in range(0, GU_M, GU_C):
        r = slice(c, c + GU_C)
        a = a_ref[r, :]
        g = dot(a, wg[n])
        u = dot(a, wu[n])
        sig = jax.nn.sigmoid(g)
        s = g * sig
        s_ref[r, :] = s
        t_ref[r, :] = u * (sig + s * (1 - sig))
        act_ref[r, :] = (s * u).astype(BF)


def gate_up(pos, a, blocks):
    out = pl.BlockSpec((GU_M, GU_N), lambda n, m, pos: (m, n))
    return pl.pallas_call(
        gu_body,
        grid_spec=pltpu.PrefetchScalarGridSpec(
            num_scalar_prefetch=1,
            grid=(GU_STEPS, T // GU_M),
            in_specs=[pl.BlockSpec((GU_M, D), lambda n, m, pos: (m, 0))] + [ANY] * 8,
            out_specs=[out] * 3,
            scratch_shapes=[
                pltpu.VMEM((GU_STEPS, D, GU_N), BF),
                pltpu.VMEM((GU_STEPS, D, GU_N), BF),
                pltpu.SemaphoreType.DMA((GU_STEPS, 16)),
            ],
        ),
        out_shape=[jax.ShapeDtypeStruct((T, HALF), d) for d in (BF, F32, F32)],
        compiler_params=params(),
        cost_estimate=cost(4 * T * D * HALF, 70_000_000),
        name="gate_up",
    )(pos, a, *blocks)


def norm_of(wide):
    return lax.rsqrt(jnp.mean(wide * wide, -1, keepdims=True) + 1e-6)


def normed(h, a_ref, at_ref):
    wide = h.astype(F32)
    a = (wide * norm_of(wide)).astype(BF)
    a_ref[...] = a
    at_ref[...] = a.astype(F32).T.astype(BF)


def norm_body(h_ref, a_ref, at_ref):
    normed(h_ref[...], a_ref, at_ref)


def norm(h):
    row = pl.BlockSpec((DN_M, D), lambda m: (m, 0))
    return pl.pallas_call(
        norm_body,
        grid=(T // DN_M,),
        in_specs=[row],
        out_specs=[row, pl.BlockSpec((D, DN_M), lambda m: (0, m))],
        out_shape=[jax.ShapeDtypeStruct((T, D), BF), jax.ShapeDtypeStruct((D, T), BF)],
        compiler_params=params(),
        cost_estimate=cost(1_000_000_000, 14_000_000),
        name="norm",
    )(h)


DN_M = 512


def down_body(pos, aa, ab, h_ref, *refs):
    blocks, (h1_ref, a1_ref, at_ref, wd, sem) = refs[:8], refs[8:]

    @pl.when(pl.program_id(0) == 0)
    def _():
        cs = [
            pltpu.make_async_copy(b, wd.at[pl.ds(pl.multiple_of(pos[j] * RF, 16), RF), :], sem.at[j])
            for j, b in enumerate(blocks)
        ]
        for c in cs:
            c.start()
        for c in cs:
            c.wait()

    out = dot(aa[...], wd[:HALF]) + dot(ab[...], wd[HALF:])
    h1 = (h_ref[...].astype(F32) + out.astype(BF).astype(F32)).astype(BF)
    h1_ref[...] = h1
    normed(h1, a1_ref, at_ref)


def down(pos, aa, ab, h, blocks):
    row = lambda n: pl.BlockSpec((DN_M, n), lambda m, pos: (m, 0))
    return pl.pallas_call(
        down_body,
        grid_spec=pltpu.PrefetchScalarGridSpec(
            num_scalar_prefetch=1,
            grid=(T // DN_M,),
            in_specs=[row(HALF), row(HALF), row(D)] + [ANY] * 8,
            out_specs=[row(D), row(D), pl.BlockSpec((D, DN_M), lambda m, pos: (0, m))],
            scratch_shapes=[pltpu.VMEM((FF, D), BF), pltpu.SemaphoreType.DMA((8,))],
        ),
        out_shape=[jax.ShapeDtypeStruct((T, D), BF)] * 2 + [jax.ShapeDtypeStruct((D, T), BF)],
        compiler_params=params(),
        cost_estimate=cost(2 * T * D * FF, 45_000_000),
        name="down",
    )(pos, aa, ab, h, *blocks)


def by_down_body(aa, ab, dh_ref, out_ref):
    c = pl.program_id(0)

    @pl.when(c < 2)
    def _():
        out_ref[...] = dot(aa[...], dh_ref[...], TN).astype(BF)

    @pl.when(c >= 2)
    def _():
        out_ref[...] = dot(ab[...], dh_ref[...], TN).astype(BF)


def by_down(aa, ab, dh):
    return pl.pallas_call(
        by_down_body,
        grid=(4,),
        in_specs=[
            pl.BlockSpec((T, D), lambda c: (0, jnp.minimum(c, 1))),
            pl.BlockSpec((T, D), lambda c: (0, jnp.maximum(c - 2, 0))),
            pl.BlockSpec((T, D), lambda c: (0, 0)),
        ],
        out_specs=pl.BlockSpec((D, D), lambda c: (c, 0)),
        out_shape=jax.ShapeDtypeStruct((FF, D), BF),
        compiler_params=params(),
        cost_estimate=cost(2 * T * D * FF, 35_000_000),
        name="by_down",
    )(aa, ab, dh)


BG_N, BG_C = 256, 512


def by_gate_up_body(half, slots, pos, dh_ref, s_ref, t_ref, at_ref, *refs):
    blocks, (dg_ref, du_ref, out, wd, sem) = refs[:8], refs[8:]
    n = pl.program_id(0)

    def each(what):
        for j, b in enumerate(blocks):

            @pl.when(pos[j] // 4 == half)
            def _():
                rows = pl.ds(pl.multiple_of((pos[j] % 4) * RF, 16), RF)
                what(pltpu.make_async_copy(b, wd.at[rows, :], sem.at[j]))

    @pl.when(n == 0)
    def _():
        each(lambda c: c.start())
        each(lambda c: c.wait())

    w = wd[pl.ds(pl.multiple_of(n * BG_N, BG_N), BG_N), :]
    for c in range(0, T, BG_C):
        r = slice(c, c + BG_C)
        d = dot(dh_ref[r, :], w, NT).astype(BF).astype(F32)
        dg_ref[r, :] = (d * t_ref[r, :]).astype(BF)
        du_ref[r, :] = (d * s_ref[r, :]).astype(BF)
    for k, v in enumerate((dg_ref, du_ref)):
        res = dot(at_ref[...], v[...]).astype(BF)
        for b in range(8):
            out[pos[8 + b] if slots else b, k * RD : (k + 1) * RD, :] = res[b * RD : (b + 1) * RD]


def by_gate_up(pos, half, slots, dh, s, t, at, blocks):
    full = lambda shape: pl.BlockSpec(shape, lambda n, pos: (0,) * len(shape), pipeline_mode=pl.Buffered(1))
    col = pl.BlockSpec((T, BG_N), lambda n, pos: (0, n))
    grad = pl.BlockSpec((8, 2 * RD, BG_N), lambda n, pos: (0, 0, n))
    return pl.pallas_call(
        functools.partial(by_gate_up_body, half, slots),
        grid_spec=pltpu.PrefetchScalarGridSpec(
            num_scalar_prefetch=1,
            grid=(HALF // BG_N,),
            in_specs=[full((T, D)), col, col, full((D, T))] + [ANY] * 8,
            out_specs=[col, col, grad],
            scratch_shapes=[pltpu.VMEM((HALF, D), BF), pltpu.SemaphoreType.DMA((8,))],
        ),
        out_shape=[jax.ShapeDtypeStruct((T, HALF), BF)] * 2 + [jax.ShapeDtypeStruct((8, 2 * RD, HALF), BF)],
        compiler_params=params(),
        cost_estimate=cost(6 * T * D * HALF, 85_000_000),
    )(pos, dh, s, t, at, *blocks)


DA_M = 512


def by_a_body(part, pos, ga, gb, *refs):
    extra, blocks, (out_ref, wa, wb, sem) = refs[:-20], refs[-20:-4], refs[-4:]
    first_step = pl.program_id(0) == 0

    def copies(k, w):
        return [
            pltpu.make_async_copy(
                blocks[8 * k + j].at[pl.ds(part * RD, RD), :],
                w.at[pl.ds(pl.multiple_of(pos[j] * RD, 16), RD), :],
                sem.at[k, j],
            )
            for j in range(8)
        ]

    @pl.when(first_step)
    def _():
        for c in copies(0, wa) + copies(1, wb):
            c.start()
        for c in copies(0, wa):
            c.wait()

    da = dot(ga[...], wa[...], NT)

    @pl.when(first_step)
    def _():
        for c in copies(1, wb):
            c.wait()

    da = (da + dot(gb[...], wb[...], NT)).astype(BF)
    if not extra:
        out_ref[...] = da
        return
    before, h_ref, dh_ref = extra
    da = (da.astype(F32) + before[...].astype(F32)).astype(BF).astype(F32)
    wide = h_ref[...].astype(F32)
    scale = norm_of(wide)
    along = jnp.mean(da * wide, -1, keepdims=True)
    by_h = (scale * da - wide * (scale * scale * scale * along)).astype(BF)
    out_ref[...] = (dh_ref[...].astype(F32) + by_h.astype(F32)).astype(BF)


def by_a(pos, part, ga, gb, blocks_a, blocks_b, extra=()):
    row = lambda n: pl.BlockSpec((DA_M, n), lambda m, pos: (m, 0))
    return pl.pallas_call(
        functools.partial(by_a_body, part),
        grid_spec=pltpu.PrefetchScalarGridSpec(
            num_scalar_prefetch=1,
            grid=(T // DA_M,),
            in_specs=[row(HALF), row(HALF)] + [row(D)] * len(extra) + [ANY] * 16,
            out_specs=row(D),
            scratch_shapes=[pltpu.VMEM((D, HALF), BF), pltpu.VMEM((D, HALF), BF), pltpu.SemaphoreType.DMA((2, 8))],
        ),
        out_shape=jax.ShapeDtypeStruct((T, D), BF),
        compiler_params=params(),
        cost_estimate=cost(2 * T * D * FF, 45_000_000),
    )(pos, ga, gb, *extra, *blocks_a, *blocks_b)


def after(v, *others):
    return lax.optimization_barrier((v, *others))[0]


def gather_ahead(v):
    return send(v, first), send(v, second)


def gather_rest(v, one, two):
    across = send(one, second)
    near = [send(b, partner) for b in (v, one, two)]
    return [v, one, two, across, *near, send(across, partner)]


def by_hand(terms):
    own, part = terms[:4], terms[4:]
    got = send(part, partner)
    pair = lambda k: own[k].astype(F32) + got[k].astype(F32)
    across = send(pair(1).astype(BF), first)
    one = send(pair(2).astype(BF), first)
    two = send((pair(3) + across.astype(F32)).astype(BF), second)
    return (pair(0) + one.astype(F32) + two.astype(F32)).astype(BF)


def scatter(terms):
    return lax.psum_scatter(terms.reshape(-1, terms.shape[-1]), "dp", scatter_dimension=0, tiled=True)


def solution(mesh):
    def whole_step(x, dy, w_gate, w_up, w_down):
        x, dy = x[0], dy[0]
        pos = places()
        units = []
        for layer in range(2):
            for half in range(2):
                cols = slice(half * HALF, (half + 1) * HALF)
                units.append(jnp.concatenate([w_gate[layer][:, cols], w_up[layer][:, cols]], 0))
            units.append(w_down[layer])
        ahead, whole = [], []
        for k, v in enumerate(units):
            if k >= 2:
                v = after(v, *ahead[k - (1 if k == 5 else 2)])
            ahead.append(gather_ahead(v))
            units[k] = v
        for v, (one, two) in zip(units, ahead):
            whole.append(gather_rest(v, one, two))
        g0a, g0b, d0, g1a, g1b, d1 = whole

        a0, at0 = norm(x)
        act0a, s0a, t0a = gate_up(pos, a0, g0a)
        act0b, s0b, t0b = gate_up(pos, after(a0, act0a), g0b)
        h1, a1, at1 = down(pos, act0a, act0b, x, d0)
        act1a, s1a, t1a = gate_up(pos, a1, g1a)
        act1b, s1b, t1b = gate_up(pos, after(a1, act1a), g1b)

        def backward(i, dh, h, at, acts, s, t, ga, gb, d):
            by_d = by_down(*acts, dh)
            later = after(dh, by_d)
            dga, dua, by_ga = by_gate_up(pos, 0, False, later, s[0], t[0], at, d)
            later = after(later, by_ga)
            dgb, dub, by_gb = by_gate_up(pos, 1, i == 0, later, s[1], t[1], at, d)
            da = by_a(pos, 0, dga, dgb, ga, gb)
            dh = by_a(pos, 1, dua, dub, ga, gb, (da, h, dh))
            return dh, (scatter(by_d), scatter(by_ga), scatter(by_gb) if i else by_hand(by_gb))

        dh, (gd1, gg1a, gg1b) = backward(1, dy, h1, at1, (act1a, act1b), (s1a, s1b), (t1a, t1b), g1a, g1b, d1)
        dx, (gd0, gg0a, gg0b) = backward(0, dh, x, at0, (act0a, act0b), (s0a, s0b), (t0a, t0b), g0a, g0b, d0)
        by_gate = jnp.stack([jnp.concatenate([p[:RD], q[:RD]], 1) for p, q in ((gg0a, gg0b), (gg1a, gg1b))])
        by_up = jnp.stack([jnp.concatenate([p[RD:], q[RD:]], 1) for p, q in ((gg0a, gg0b), (gg1a, gg1b))])
        return dx[None], by_gate, by_up, jnp.stack([gd0, gd1])

    tokens, rows = P(("rep", "dp"), None, None), P(None, "dp", None)
    return jax.shard_map(
        whole_step,
        mesh=mesh,
        in_specs=(tokens, tokens, rows, rows, rows),
        out_specs=(tokens, *(P("rep", "dp", None),) * 3),
        check_vma=False,
    )
```

```python
import functools

import jax
import jax.numpy as jnp
from jax import lax
from jax.experimental import pallas as pl
from jax.experimental.pallas import tpu as pltpu
from jax.sharding import PartitionSpec as P


T, D, FF = 2048, 1152, 4608
HALF = FF // 2
RD = D // 8
RF = FF // 8
BF, F32 = jnp.bfloat16, jnp.float32
VMEM_LIMIT = 67_043_328
NT = (((1,), (1,)), ((), ()))
TN = (((0,), (0,)), ((), ()))
ANY = pl.BlockSpec(memory_space=pl.ANY)


def first(i):
    return i ^ (4 if i % 2 == 0 else 2)


def second(i):
    return i ^ (2 if i % 2 == 0 else 4)


def partner(i):
    return i ^ 1


def send(v, to):
    return lax.ppermute(v, "dp", [(i, to(i)) for i in range(8)])


def dot(a, b, dims=None):
    if dims is None:
        return jnp.dot(a, b, preferred_element_type=F32)
    return lax.dot_general(a, b, dims, preferred_element_type=F32)


def params(**kw):
    return pltpu.CompilerParams(vmem_limit_bytes=VMEM_LIMIT, **kw)


def cost(flops, nbytes):
    return pl.CostEstimate(flops=flops, bytes_accessed=nbytes, transcendentals=0)


def places():
    me = lax.axis_index("dp")
    core = me % 2
    one, two = 4 - 2 * core, 2 + 2 * core
    other = me ^ 1
    where = [me, me ^ one, me ^ two, me ^ 6, other, other ^ two, other ^ one, other ^ 6]
    slots = []
    for b in range(8):
        chips = (b ^ me) // 2
        ahead = 2 if b % 2 == 0 else 1
        slot = jnp.where(chips == 0, 0, jnp.where(chips == 3, 1, jnp.where(chips == ahead, 2, 3)))
        slots.append(slot + 4 * ((b ^ me) % 2))
    return jnp.stack([v.astype(jnp.int32) for v in (*where, *slots)])


GU_M, GU_N, GU_C = 512, 768, 512
GU_STEPS = HALF // GU_N


def gu_body(pos, a_ref, *refs):
    blocks, (act_ref, s_ref, t_ref, wg, wu, sem) = refs[:8], refs[8:]
    n, m = pl.program_id(0), pl.program_id(1)

    def copies(k):
        cols = pl.ds(k * GU_N, GU_N)
        out = []
        for j, block in enumerate(blocks):
            rows = pl.ds(pl.multiple_of(pos[j] * RD, 16), RD)
            out.append(pltpu.make_async_copy(block.at[pl.ds(0, RD), cols], wg.at[k, rows, :], sem.at[k, 2 * j]))
            out.append(pltpu.make_async_copy(block.at[pl.ds(RD, RD), cols], wu.at[k, rows, :], sem.at[k, 2 * j + 1]))
        return out

    @pl.when((n == 0) & (m == 0))
    def _():
        for k in range(GU_STEPS):
            for c in copies(k):
                c.start()

    for k in range(GU_STEPS):

        @pl.when((n == k) & (m == 0))
        def _():
            for c in copies(k):
                c.wait()

    for c in range(0, GU_M, GU_C):
        r = slice(c, c + GU_C)
        a = a_ref[r, :]
        g = dot(a, wg[n])
        u = dot(a, wu[n])
        sig = jax.nn.sigmoid(g)
        s = g * sig
        s_ref[r, :] = s
        t_ref[r, :] = u * (sig + s * (1 - sig))
        act_ref[r, :] = (s * u).astype(BF)


def gate_up(pos, a, blocks):
    out = pl.BlockSpec((GU_M, GU_N), lambda n, m, pos: (m, n))
    return pl.pallas_call(
        gu_body,
        grid_spec=pltpu.PrefetchScalarGridSpec(
            num_scalar_prefetch=1,
            grid=(GU_STEPS, T // GU_M),
            in_specs=[pl.BlockSpec((GU_M, D), lambda n, m, pos: (m, 0))] + [ANY] * 8,
            out_specs=[out] * 3,
            scratch_shapes=[
                pltpu.VMEM((GU_STEPS, D, GU_N), BF),
                pltpu.VMEM((GU_STEPS, D, GU_N), BF),
                pltpu.SemaphoreType.DMA((GU_STEPS, 16)),
            ],
        ),
        out_shape=[jax.ShapeDtypeStruct((T, HALF), d) for d in (BF, F32, F32)],
        compiler_params=params(),
        cost_estimate=cost(4 * T * D * HALF, 70_000_000),
        name="gate_up",
    )(pos, a, *blocks)


def norm_of(wide):
    return lax.rsqrt(jnp.mean(wide * wide, -1, keepdims=True) + 1e-6)


def normed(h, a_ref, at_ref):
    wide = h.astype(F32)
    a = (wide * norm_of(wide)).astype(BF)
    a_ref[...] = a
    at_ref[...] = a.astype(F32).T.astype(BF)


def norm_body(h_ref, a_ref, at_ref):
    normed(h_ref[...], a_ref, at_ref)


def norm(h):
    row = pl.BlockSpec((DN_M, D), lambda m: (m, 0))
    return pl.pallas_call(
        norm_body,
        grid=(T // DN_M,),
        in_specs=[row],
        out_specs=[row, pl.BlockSpec((D, DN_M), lambda m: (0, m))],
        out_shape=[jax.ShapeDtypeStruct((T, D), BF), jax.ShapeDtypeStruct((D, T), BF)],
        compiler_params=params(),
        cost_estimate=cost(1_000_000_000, 14_000_000),
        name="norm",
    )(h)


DN_M = 512


def down_body(pos, aa, ab, h_ref, *refs):
    blocks, (h1_ref, a1_ref, at_ref, wd, sem) = refs[:8], refs[8:]

    @pl.when(pl.program_id(0) == 0)
    def _():
        cs = [
            pltpu.make_async_copy(b, wd.at[pl.ds(pl.multiple_of(pos[j] * RF, 16), RF), :], sem.at[j])
            for j, b in enumerate(blocks)
        ]
        for c in cs:
            c.start()
        for c in cs:
            c.wait()

    out = dot(aa[...], wd[:HALF]) + dot(ab[...], wd[HALF:])
    h1 = (h_ref[...].astype(F32) + out.astype(BF).astype(F32)).astype(BF)
    h1_ref[...] = h1
    normed(h1, a1_ref, at_ref)


def down(pos, aa, ab, h, blocks):
    row = lambda n: pl.BlockSpec((DN_M, n), lambda m, pos: (m, 0))
    return pl.pallas_call(
        down_body,
        grid_spec=pltpu.PrefetchScalarGridSpec(
            num_scalar_prefetch=1,
            grid=(T // DN_M,),
            in_specs=[row(HALF), row(HALF), row(D)] + [ANY] * 8,
            out_specs=[row(D), row(D), pl.BlockSpec((D, DN_M), lambda m, pos: (0, m))],
            scratch_shapes=[pltpu.VMEM((FF, D), BF), pltpu.SemaphoreType.DMA((8,))],
        ),
        out_shape=[jax.ShapeDtypeStruct((T, D), BF)] * 2 + [jax.ShapeDtypeStruct((D, T), BF)],
        compiler_params=params(),
        cost_estimate=cost(2 * T * D * FF, 45_000_000),
        name="down",
    )(pos, aa, ab, h, *blocks)


def by_down_body(aa, ab, dh_ref, out_ref):
    c = pl.program_id(0)

    @pl.when(c < 2)
    def _():
        out_ref[...] = dot(aa[...], dh_ref[...], TN).astype(BF)

    @pl.when(c >= 2)
    def _():
        out_ref[...] = dot(ab[...], dh_ref[...], TN).astype(BF)


def by_down(aa, ab, dh):
    return pl.pallas_call(
        by_down_body,
        grid=(4,),
        in_specs=[
            pl.BlockSpec((T, D), lambda c: (0, jnp.minimum(c, 1))),
            pl.BlockSpec((T, D), lambda c: (0, jnp.maximum(c - 2, 0))),
            pl.BlockSpec((T, D), lambda c: (0, 0)),
        ],
        out_specs=pl.BlockSpec((D, D), lambda c: (c, 0)),
        out_shape=jax.ShapeDtypeStruct((FF, D), BF),
        compiler_params=params(),
        cost_estimate=cost(2 * T * D * FF, 35_000_000),
        name="by_down",
    )(aa, ab, dh)


BG_N, BG_C = 256, 512


def by_gate_up_body(half, slots, pos, dh_ref, s_ref, t_ref, at_ref, *refs):
    blocks, (dg_ref, du_ref, out, wd, sem) = refs[:8], refs[8:]
    n = pl.program_id(0)

    def each(what):
        for j, b in enumerate(blocks):

            @pl.when(pos[j] // 4 == half)
            def _():
                rows = pl.ds(pl.multiple_of((pos[j] % 4) * RF, 16), RF)
                what(pltpu.make_async_copy(b, wd.at[rows, :], sem.at[j]))

    @pl.when(n == 0)
    def _():
        each(lambda c: c.start())

    for j, b in enumerate(blocks):
        k = pos[j] - 4 * half

        @pl.when((k >= 0) & (k < 4) & (n == k * RF // BG_N))
        def _():
            rows = pl.ds(pl.multiple_of(k * RF, 16), RF)
            pltpu.make_async_copy(b, wd.at[rows, :], sem.at[j]).wait()

    w = wd[pl.ds(pl.multiple_of(n * BG_N, BG_N), BG_N), :]
    for c in range(0, T, BG_C):
        r = slice(c, c + BG_C)
        d = dot(dh_ref[r, :], w, NT).astype(BF).astype(F32)
        dg_ref[r, :] = (d * t_ref[r, :]).astype(BF)
        du_ref[r, :] = (d * s_ref[r, :]).astype(BF)
    for k, v in enumerate((dg_ref, du_ref)):
        res = dot(at_ref[...], v[...]).astype(BF)
        for b in range(8):
            out[pos[8 + b] if slots else b, k * RD : (k + 1) * RD, :] = res[b * RD : (b + 1) * RD]


def by_gate_up(pos, half, slots, dh, s, t, at, blocks):
    full = lambda shape: pl.BlockSpec(shape, lambda n, pos: (0,) * len(shape), pipeline_mode=pl.Buffered(1))
    col = pl.BlockSpec((T, BG_N), lambda n, pos: (0, n))
    grad = pl.BlockSpec((8, 2 * RD, BG_N), lambda n, pos: (0, 0, n))
    return pl.pallas_call(
        functools.partial(by_gate_up_body, half, slots),
        grid_spec=pltpu.PrefetchScalarGridSpec(
            num_scalar_prefetch=1,
            grid=(HALF // BG_N,),
            in_specs=[full((T, D)), col, col, full((D, T))] + [ANY] * 8,
            out_specs=[col, col, grad],
            scratch_shapes=[pltpu.VMEM((HALF, D), BF), pltpu.SemaphoreType.DMA((8,))],
        ),
        out_shape=[jax.ShapeDtypeStruct((T, HALF), BF)] * 2 + [jax.ShapeDtypeStruct((8, 2 * RD, HALF), BF)],
        compiler_params=params(),
        cost_estimate=cost(6 * T * D * HALF, 85_000_000),
    )(pos, dh, s, t, at, *blocks)


DA_M = 512


def by_a_body(part, pos, ga, gb, *refs):
    extra, blocks, (out_ref, wa, wb, sem) = refs[:-20], refs[-20:-4], refs[-4:]
    first_step = pl.program_id(0) == 0

    def copies(k, w):
        return [
            pltpu.make_async_copy(
                blocks[8 * k + j].at[pl.ds(part * RD, RD), :],
                w.at[pl.ds(pl.multiple_of(pos[j] * RD, 16), RD), :],
                sem.at[k, j],
            )
            for j in range(8)
        ]

    @pl.when(first_step)
    def _():
        for c in copies(0, wa) + copies(1, wb):
            c.start()
        for c in copies(0, wa):
            c.wait()

    da = dot(ga[...], wa[...], NT)

    @pl.when(first_step)
    def _():
        for c in copies(1, wb):
            c.wait()

    da = (da + dot(gb[...], wb[...], NT)).astype(BF)
    if not extra:
        out_ref[...] = da
        return
    before, h_ref, dh_ref = extra
    da = (da.astype(F32) + before[...].astype(F32)).astype(BF).astype(F32)
    wide = h_ref[...].astype(F32)
    scale = norm_of(wide)
    along = jnp.mean(da * wide, -1, keepdims=True)
    by_h = (scale * da - wide * (scale * scale * scale * along)).astype(BF)
    out_ref[...] = (dh_ref[...].astype(F32) + by_h.astype(F32)).astype(BF)


def by_a(pos, part, ga, gb, blocks_a, blocks_b, extra=()):
    row = lambda n: pl.BlockSpec((DA_M, n), lambda m, pos: (m, 0))
    return pl.pallas_call(
        functools.partial(by_a_body, part),
        grid_spec=pltpu.PrefetchScalarGridSpec(
            num_scalar_prefetch=1,
            grid=(T // DA_M,),
            in_specs=[row(HALF), row(HALF)] + [row(D)] * len(extra) + [ANY] * 16,
            out_specs=row(D),
            scratch_shapes=[pltpu.VMEM((D, HALF), BF), pltpu.VMEM((D, HALF), BF), pltpu.SemaphoreType.DMA((2, 8))],
        ),
        out_shape=jax.ShapeDtypeStruct((T, D), BF),
        compiler_params=params(),
        cost_estimate=cost(2 * T * D * FF, 45_000_000),
    )(pos, ga, gb, *extra, *blocks_a, *blocks_b)


def lay_body(*refs):
    pieces, (g_ref, u_ref, d_ref) = refs[:6], refs[6:]
    for layer in range(2):

        @pl.when(pl.program_id(0) == 1 - layer)
        def _():
            for half in range(2):
                piece = pieces[3 * layer + half]
                g_ref[0, :, half * HALF : (half + 1) * HALF] = piece[:RD]
                u_ref[0, :, half * HALF : (half + 1) * HALF] = piece[RD:]
            d_ref[0] = pieces[3 * layer + 2][...]


def lay(pieces):
    out = lambda rows, cols: pl.BlockSpec((1, rows, cols), lambda i: (1 - i, 0, 0))
    return pl.pallas_call(
        lay_body,
        grid=(2,),
        in_specs=[pl.BlockSpec(p.shape, lambda i: (0, 0)) for p in pieces],
        out_specs=[out(RD, FF), out(RD, FF), out(RF, D)],
        out_shape=[jax.ShapeDtypeStruct((2, *s), BF) for s in ((RD, FF), (RD, FF), (RF, D))],
        compiler_params=params(),
        cost_estimate=cost(1_000_000, 16_000_000),
        name="lay",
    )(*pieces)


def after(v, *others):
    return lax.optimization_barrier((v, *others))[0]


def gather_ahead(v):
    return send(v, first), send(v, second)


def gather_rest(v, one, two):
    across = send(one, second)
    near = [send(b, partner) for b in (v, one, two)]
    return [v, one, two, across, *near, send(across, partner)]


def by_hand(terms):
    own, got = terms[:4], send(terms, partner)[4:]
    pair = lambda k: own[k].astype(F32) + got[k].astype(F32)
    across = send(pair(1).astype(BF), first)
    one = send(pair(2).astype(BF), first)
    two = send((pair(3) + across.astype(F32)).astype(BF), second)
    return (pair(0) + one.astype(F32) + two.astype(F32)).astype(BF)


def scatter(terms):
    return lax.psum_scatter(terms.reshape(-1, terms.shape[-1]), "dp", scatter_dimension=0, tiled=True)


def solution(mesh):
    def whole_step(x, dy, w_gate, w_up, w_down):
        x, dy = x[0], dy[0]
        pos = places()
        units = []
        for layer in range(2):
            for half in range(2):
                cols = slice(half * HALF, (half + 1) * HALF)
                units.append(jnp.concatenate([w_gate[layer][:, cols], w_up[layer][:, cols]], 0))
            units.append(w_down[layer])
        ahead, whole = [], []
        for k, v in enumerate(units):
            if k >= 2:
                v = after(v, *ahead[k - (1 if k == 5 else 2)])
            ahead.append(gather_ahead(v))
            units[k] = v
        for v, (one, two) in zip(units, ahead):
            whole.append(gather_rest(v, one, two))
        g0a, g0b, d0, g1a, g1b, d1 = whole

        a0, at0 = norm(x)
        act0a, s0a, t0a = gate_up(pos, a0, g0a)
        act0b, s0b, t0b = gate_up(pos, after(a0, act0a), g0b)
        h1, a1, at1 = down(pos, act0a, act0b, x, d0)
        act1a, s1a, t1a = gate_up(pos, a1, g1a)
        act1b, s1b, t1b = gate_up(pos, after(a1, act1a), g1b)

        def backward(i, dh, h, at, acts, s, t, ga, gb, d):
            by_d = by_down(*acts, dh)
            later = after(dh, by_d)
            dga, dua, by_ga = by_gate_up(pos, 0, i == 0, later, s[0], t[0], at, d)
            later = after(later, by_ga)
            dgb, dub, by_gb = by_gate_up(pos, 1, False, later, s[1], t[1], at, d)
            da = by_a(pos, 0, dga, dgb, ga, gb)
            dh = by_a(pos, 1, dua, dub, ga, gb, (da, h, dh))
            return dh, (scatter(by_d), scatter(by_ga) if i else by_hand(by_ga), scatter(by_gb))

        dh, (gd1, gg1a, gg1b) = backward(1, dy, h1, at1, (act1a, act1b), (s1a, s1b), (t1a, t1b), g1a, g1b, d1)
        dx, (gd0, gg0a, gg0b) = backward(0, dh, x, at0, (act0a, act0b), (s0a, s0b), (t0a, t0b), g0a, g0b, d0)
        return dx[None], *lay((gg0a, gg0b, gd0, gg1a, gg1b, gd1))

    tokens, rows = P(("rep", "dp"), None, None), P(None, "dp", None)
    return jax.shard_map(
        whole_step,
        mesh=mesh,
        in_specs=(tokens, tokens, rows, rows, rows),
        out_specs=(tokens, *(P("rep", "dp", None),) * 3),
        check_vma=False,
    )
```
